32 devices in a mesh: dp: 8 (over y, x, core), fsdp: 4 (over z).
Axes of the slice: x: 2, y: 2, z: 4, core: 2. Of those that a mesh axis runs over, the one named last changes fastest.
Arguments:
- latents: bfloat16 [2, 32, 4, 1024], P(None, ('dp', 'fsdp')), may hold values from -6 to 6
- noise: bfloat16 [2, 32, 4, 1024], P(None, ('dp', 'fsdp')), may hold values from -6 to 6
- context: bfloat16 [2, 32, 77, 768], P(None, ('dp', 'fsdp')), may hold values from -6 to 6
- timesteps: int32 [2, 32], P(None, ('dp', 'fsdp')), may hold values from 0 to 999
- region_mask: int32 [2, 32, 1024], P(None, ('dp', 'fsdp')), may hold values from 0 to 1, as said below
- owners: int32 [8], replicated, may hold values from 0 to 7, each once
- step_count: int32 [1], replicated, may hold values from 2 to 20
- kernels_weight: float32 [2, 2880, 320], P(None, 'dp', 'fsdp'), may hold values from -0.109375 to 0.109375
- kernels_first: float32 [2, 2880, 320], P(None, 'dp', 'fsdp'), may hold values from -6.4818124e-07 to 6.4818124e-07
- kernels_second: float32 [2, 2880, 320], P(None, 'dp', 'fsdp'), may hold values from 2.1701389e-15 to 8.6805554e-15
- entry_weight: float32 [320, 1280], P('dp', 'fsdp'), may hold values from -0.3125 to 0.3125
- entry_first: float32 [320, 1280], P('dp', 'fsdp'), may hold values from -6.875e-08 to 6.875e-08
- entry_second: float32 [320, 1280], P('dp', 'fsdp'), may hold values from 2.4414062e-17 to 9.765625e-17
- middle_weight: float32 [1280, 1280], P('dp', 'fsdp'), may hold values from -0.15625 to 0.15625
- middle_first: float32 [1280, 1280], P('dp', 'fsdp'), may hold values from -4.8125e-08 to 4.8125e-08
- middle_second: float32 [1280, 1280], P('dp', 'fsdp'), may hold values from 1.196289e-17 to 4.785156e-17
- narrow_weight: float32 [2, 1280, 320], P(None, 'dp', 'fsdp'), may hold values from -0.15625 to 0.15625
- narrow_first: float32 [2, 1280, 320], P(None, 'dp', 'fsdp'), may hold values from -1.1667262e-07 to 1.1667262e-07
- narrow_second: float32 [2, 1280, 320], P(None, 'dp', 'fsdp'), may hold values from 7.03125e-17 to 2.8125e-16
- crossing_weight: float32 [768, 640], P('dp', 'fsdp'), may hold values from -0.21875 to 0.21875
- crossing_first: float32 [768, 640], P('dp', 'fsdp'), may hold values from -4.518711e-08 to 4.518711e-08
- crossing_second: float32 [768, 640], P('dp', 'fsdp'), may hold values from 1.0546875e-17 to 4.21875e-17
- widen_weight: float32 [320, 2560], P('dp', 'fsdp'), may hold values from -0.3125 to 0.3125
- widen_first: float32 [320, 2560], P('dp', 'fsdp'), may hold values from -3.0140427e-08 to 3.0140427e-08
- widen_second: float32 [320, 2560], P('dp', 'fsdp'), may hold values from 4.6923826e-18 to 1.876953e-17
- vectors_weight: float32 [112, 320], P('dp', 'fsdp'), as said below
- vectors_first: float32 [112, 320], P('dp', 'fsdp'), may hold values from -4.6483483e-06 to 4.6483483e-06
- vectors_second: float32 [112, 320], P('dp', 'fsdp'), may hold values from 1.1160714e-13 to 4.4642857e-13
- squares_weight: float32 [8, 320, 320], P(None, 'dp', 'fsdp')
- squares_state: float32 [6, 8, 320, 320], P(None, 'fsdp'), as said below
Outputs:
- totals: float32 [2], replicated
- kernels_master: float32 [2, 2880, 320], P(None, 'dp', 'fsdp')
- kernels_moment: float32 [2, 2880, 320], P(None, 'dp', 'fsdp')
- kernels_variance: float32 [2, 2880, 320], P(None, 'dp', 'fsdp')
- entry_master: float32 [320, 1280], P('dp', 'fsdp')
- entry_moment: float32 [320, 1280], P('dp', 'fsdp')
- entry_variance: float32 [320, 1280], P('dp', 'fsdp')
- middle_master: float32 [1280, 1280], P('dp', 'fsdp')
- middle_moment: float32 [1280, 1280], P('dp', 'fsdp')
- middle_variance: float32 [1280, 1280], P('dp', 'fsdp')
- narrow_master: float32 [2, 1280, 320], P(None, 'dp', 'fsdp')
- narrow_moment: float32 [2, 1280, 320], P(None, 'dp', 'fsdp')
- narrow_variance: float32 [2, 1280, 320], P(None, 'dp', 'fsdp')
- crossing_master: float32 [768, 640], P('dp', 'fsdp')
- crossing_moment: float32 [768, 640], P('dp', 'fsdp')
- crossing_variance: float32 [768, 640], P('dp', 'fsdp')
- widen_master: float32 [320, 2560], P('dp', 'fsdp')
- widen_moment: float32 [320, 2560], P('dp', 'fsdp')
- widen_variance: float32 [320, 2560], P('dp', 'fsdp')
- vectors_master: float32 [112, 320], P('dp', 'fsdp')
- vectors_moment: float32 [112, 320], P('dp', 'fsdp')
- vectors_variance: float32 [112, 320], P('dp', 'fsdp')
- squares_master: float32 [8, 320, 320], P(None, 'dp', 'fsdp')
- squares_slots: float32 [2, 8, 320, 320], P(None, 'fsdp')
- squares_grad: float32 [8, 320, 320], P('fsdp')
The draws below stay inside these ranges and needn't reach their ends.
Inputs may be any that keep to these rules, and one draw needn't show every extreme that they name: `region_mask`: 1 marks a pixel whose error counts; pixel 0 of every sample counts. `owners`: each slot names a different matrix; slot j is kept by the devices whose fsdp index is j // (8 // the number of fsdp devices). `vectors_weight`: rows as the steps name them. `squares_state`: in every slot the statistics L and R are symmetric positive definite and the bases QL and QR orthogonal.
All inputs are finite; a program needn't handle non-finite values.
Results may differ from the reference program's by a relative error of at most 0.012.
The reference program's roundings to bfloat16 on the way (of `noised`) count: a program that leaves them out, or rounds other values in their place, can miss the bound.
Values may be sent and summed in bfloat16 or wider, within the bound.
A program may use at most 320 MiB of HBM per device.

```python
import math
import jax
import jax.numpy as jnp
from jax import lax

C = 320
HEADS = 8
GROUPS = 32
CTX_DIM = 768
CTX_LEN = 77
SIDE = 32
MICRO = 2
NSOAP = 8
SMALL_ROWS = 112
HEAD_DIM = 40
TOK = 1024
SAMPLES = 32


def gradient_scale():
    return 0.002 / math.sqrt(NSOAP * C * C)


def draw_region_mask(key, part):
    rolls = jax.random.randint(key, (MICRO, SAMPLES, TOK), 0, 100)
    sample_index = jnp.arange(SAMPLES)[None, :, None]
    limits = 25 + 50 * sample_index // max(SAMPLES - 1, 1)
    marks = (rolls < limits).astype(jnp.int32)
    leading = (jnp.arange(TOK) == 0)[None, None, :]
    return jnp.where(leading, 1, marks).astype(jnp.int32)


def draw_vectors_weight(key, part):
    base = jax.random.truncated_normal(key, -4.0, 4.0, (SMALL_ROWS, C), jnp.float32)
    rows = jnp.arange(SMALL_ROWS)[:, None]
    gains = (rows == 73) | (rows == 85) | (rows == 88) | (rows == 91) | (rows == 94) | (rows == 97) | (rows == 109)
    scaling = jnp.where(rows < 36, 1.0 / 6.0, jnp.where(rows < 72, 1.0 / math.sqrt(9 * C), 0.2))
    scaling = jnp.where(gains, 0.1, scaling)
    return jnp.where(gains, 1.0, 0.0) + base * scaling


def draw_squares_weight(key, part):
    base = jax.random.truncated_normal(key, -4.0, 4.0, (NSOAP, C, C), jnp.float32)
    index = jnp.arange(NSOAP)
    boost = jnp.where(index == 3, math.sqrt(TOK / 4.0), jnp.where(index == 5, math.sqrt(CTX_LEN / 4.0), 1.0))
    return base * boost[:, None, None] / math.sqrt(C)


def rotation(key):
    first_key, second_key = jax.random.split(key)
    first_dir = jax.random.normal(first_key, (NSOAP, C, 1), jnp.float32)
    second_dir = jax.random.normal(second_key, (NSOAP, C, 1), jnp.float32)
    first_dir = first_dir / jnp.sqrt(jnp.sum(first_dir * first_dir, axis=1, keepdims=True))
    second_dir = second_dir / jnp.sqrt(jnp.sum(second_dir * second_dir, axis=1, keepdims=True))
    inner_value = jnp.sum(first_dir * second_dir, axis=1, keepdims=True)
    first_row = jnp.swapaxes(first_dir, 1, 2)
    second_row = jnp.swapaxes(second_dir, 1, 2)
    identity = jnp.eye(C, dtype=jnp.float32)[None]
    return identity - 2.0 * first_dir * first_row - 2.0 * second_dir * second_row + 4.0 * inner_value * first_dir * second_row


def statistic(key):
    noise_key, level_key = jax.random.split(key)
    base = jax.random.truncated_normal(noise_key, -4.0, 4.0, (NSOAP, C, C), jnp.float32)
    levels = jnp.exp(jax.random.uniform(level_key, (NSOAP, 1, 1), jnp.float32, 0.0, math.log(4.0)))
    sizes = levels * (0.05 / 0.95) * C * gradient_scale() ** 2
    identity = jnp.eye(C, dtype=jnp.float32)[None]
    return sizes * (identity + (base + jnp.swapaxes(base, 1, 2)) / (6.0 * math.sqrt(C)))


def draw_squares_state(key, part):
    keys = jax.random.split(key, 6)
    scaling = gradient_scale()
    moment = 0.11 * scaling * jax.random.truncated_normal(keys[0], -4.0, 4.0, (NSOAP, C, C), jnp.float32)
    second = scaling * scaling * jnp.exp(jax.random.uniform(keys[1], (NSOAP, C, C), jnp.float32, math.log(0.001), math.log(0.004)))
    return jnp.stack([moment, second, statistic(keys[2]), statistic(keys[3]), rotation(keys[4]), rotation(keys[5])])


def place_ends(result, rng, least, largest):
    longest = result.shape.index(max(result.shape))
    spots = []
    for shift in (0, 1):
        where = [jax.random.randint(jax.random.fold_in(rng, axis), (), 0, length) for axis, length in enumerate(result.shape)]
        where[longest] = (where[longest] + shift) % result.shape[longest]
        spots.append(tuple(where))
    return result.at[spots[0]].set(least).at[spots[1]].set(largest)


def block_scale(rng, shape, cuts, low, high):
    def one(position, blocks):
        draws = jax.random.uniform(jax.random.fold_in(jax.random.fold_in(rng, 6), position), (blocks,), jnp.float32, low / len(cuts), high / len(cuts))
        return jnp.repeat(jnp.exp(draws), shape[position] // blocks).reshape((-1,) + (1,) * (len(shape) - position - 1))

    loudness = one(*cuts[0])
    for cut in cuts[1:]:
        loudness = loudness * one(*cut)
    return loudness


def centred(stream_key, extent, width, bound, cuts=(), kind=jnp.bfloat16):
    result = jax.random.normal(stream_key, extent, jnp.float32) * width
    if len(cuts) > 0:
        result = block_scale(stream_key, extent, cuts, -0.22, 0.18) * result
    return jnp.clip(result, min=-bound, max=bound).astype(kind)


def setup_inputs(seed: int = 0) -> dict:
    splits = jax.random.split(jax.random.key(seed), 31)
    return {
        "latents": centred(splits[0], (MICRO, SAMPLES, 4, TOK), 1.0, 6.0, ((1, 32),)),
        "noise": centred(splits[1], (MICRO, SAMPLES, 4, TOK), 1.0, 6.0, ((1, 32),)),
        "context": centred(splits[2], (MICRO, SAMPLES, CTX_LEN, CTX_DIM), 1.0, 6.0, ((1, 32),)),
        "timesteps": place_ends(jax.random.randint(splits[3], (MICRO, SAMPLES), 0, 1000), jax.random.fold_in(splits[3], 1), 0, 999).astype(jnp.int32),
        "region_mask": draw_region_mask(jax.random.fold_in(splits[30], 71), 0),
        "owners": jax.random.permutation(splits[5], NSOAP).astype(jnp.int32),
        "step_count": jax.random.randint(splits[6], (1,), 2, 21).astype(jnp.int32),
        "kernels_weight": centred(splits[7], (2, 9 * C, C), (9 * C) ** -0.5, 0.109375, ((1, 8), (2, 4)), jnp.float32),
        "kernels_first": centred(splits[8], (2, 9 * C, C), (0.00022 * (18 * C * C) ** -0.5), 6.481812420133792e-07, ((1, 8), (2, 4)), jnp.float32),
        "kernels_second": jnp.clip(jnp.exp(math.log(8.680555426754995e-15) - 1.3862944 * jax.random.uniform(splits[9], (2, 9 * C, C), jnp.float32) ** block_scale(splits[9], (2, 9 * C, C), ((1, 8), (2, 4)), -0.2, 0.2)), 2.170138856688749e-15, 8.680555426754995e-15),
        "entry_weight": centred(splits[10], (C, 4 * C), C ** -0.5, 0.3125, ((0, 8), (1, 4)), jnp.float32),
        "entry_first": centred(splits[11], (C, 4 * C), (0.00022 * 0.05 * (4 * C * C) ** -0.5), 6.874999769479473e-08, ((0, 8), (1, 4)), jnp.float32),
        "entry_second": jnp.clip(jnp.exp(math.log(9.76562482862959e-17) - 1.3862944 * jax.random.uniform(splits[12], (C, 4 * C), jnp.float32) ** block_scale(splits[12], (C, 4 * C), ((0, 8), (1, 4)), -0.2, 0.2)), 2.4414062071573976e-17, 9.76562482862959e-17),
        "middle_weight": centred(splits[13], (4 * C, 4 * C), (4 * C) ** -0.5, 0.15625, ((0, 8), (1, 4)), jnp.float32),
        "middle_first": centred(splits[14], (4 * C, 4 * C), (0.00022 * 0.07 * (16 * C * C) ** -0.5), 4.8124999096899046e-08, ((0, 8), (1, 4)), jnp.float32),
        "middle_second": jnp.clip(jnp.exp(math.log(4.785156132941275e-17) - 1.3862944 * jax.random.uniform(splits[15], (4 * C, 4 * C), jnp.float32) ** block_scale(splits[15], (4 * C, 4 * C), ((0, 8), (1, 4)), -0.2, 0.2)), 1.1962890332353187e-17, 4.785156132941275e-17),
        "narrow_weight": centred(splits[16], (2, 4 * C, C), (4 * C) ** -0.5, 0.15625, ((1, 8), (2, 4)), jnp.float32),
        "narrow_first": centred(splits[17], (2, 4 * C, C), (0.00022 * 0.12 * (8 * C * C) ** -0.5), 1.166726164569809e-07, ((1, 8), (2, 4)), jnp.float32),
        "narrow_second": jnp.clip(jnp.exp(math.log(2.8125001094639996e-16) - 1.3862944 * jax.random.uniform(splits[18], (2, 4 * C, C), jnp.float32) ** block_scale(splits[18], (2, 4 * C, C), ((1, 8), (2, 4)), -0.2, 0.2)), 7.031250273659999e-17, 2.8125001094639996e-16),
        "crossing_weight": centred(splits[19], (CTX_DIM, 2 * C), CTX_DIM ** -0.5, 0.21875, ((0, 8), (1, 4)), jnp.float32),
        "crossing_first": centred(splits[20], (CTX_DIM, 2 * C), (0.00022 * 0.036 * (2 * CTX_DIM * C) ** -0.5), 4.51871109419244e-08, ((0, 8), (1, 4)), jnp.float32),
        "crossing_second": jnp.clip(jnp.exp(math.log(4.2187501641959994e-17) - 1.3862944 * jax.random.uniform(splits[21], (CTX_DIM, 2 * C), jnp.float32) ** block_scale(splits[21], (CTX_DIM, 2 * C), ((0, 8), (1, 4)), -0.2, 0.2)), 1.0546875410489999e-17, 4.2187501641959994e-17),
        "widen_weight": centred(splits[22], (C, 8 * C), C ** -0.5, 0.3125, ((0, 8), (1, 4)), jnp.float32),
        "widen_first": centred(splits[23], (C, 8 * C), (0.00022 * 0.031 * (8 * C * C) ** -0.5), 3.01404270430794e-08, ((0, 8), (1, 4)), jnp.float32),
        "widen_second": jnp.clip(jnp.exp(math.log(1.8769530464022374e-17) - 1.3862944 * jax.random.uniform(splits[24], (C, 8 * C), jnp.float32) ** block_scale(splits[24], (C, 8 * C), ((0, 8), (1, 4)), -0.2, 0.2)), 4.6923826160055936e-18, 1.8769530464022374e-17),
        "vectors_weight": draw_vectors_weight(jax.random.fold_in(splits[30], 71), 0),
        "vectors_first": centred(splits[26], (SMALL_ROWS, C), (0.00022 * (SMALL_ROWS * C) ** -0.5), 4.648348294722382e-06, ((0, 8), (1, 4)), jnp.float32),
        "vectors_second": jnp.clip(jnp.exp(math.log(4.464285657725803e-13) - 1.3862944 * jax.random.uniform(splits[27], (SMALL_ROWS, C), jnp.float32) ** block_scale(splits[27], (SMALL_ROWS, C), ((0, 8), (1, 4)), -0.2, 0.2)), 1.1160714144314507e-13, 4.464285657725803e-13),
        "squares_weight": draw_squares_weight(jax.random.fold_in(splits[30], 71), 0),
        "squares_state": draw_squares_state(jax.random.fold_in(splits[30], 71), 0),
    }


highest = lax.Precision.HIGHEST
beta_one = 0.9
beta_two = 0.999
beta_stat = 0.95
adam_eps = 1e-08
decay = 0.01
clip_limit = 0.002

@jax.custom_vjp
def low(v):
    return lax.optimization_barrier(v.astype(jnp.bfloat16)).astype(jnp.float32)

@jax.custom_vjp
def low_back(v):
    return v

def low_keep(v):
    return (low(v), None)

def low_pass(kept, grad):
    return (grad,)

def back_keep(v):
    return (v, None)

def back_low(kept, grad):
    return (low(grad),)
low.defvjp(low_keep, low_pass)
low_back.defvjp(back_keep, back_low)

def product(left_matrix, right_matrix):
    return jnp.dot(left_matrix, right_matrix, precision=highest)

def rates():
    return (3.0 / math.sqrt(9 * C), 3.0 / math.sqrt(C), 3.0 / math.sqrt(4 * C), 3.0 / math.sqrt(4 * C), 3.0 / math.sqrt(CTX_DIM), 3.0 / math.sqrt(C), 0.3, 3.0 / math.sqrt(C))

def noise_level(timestep):
    levels = jnp.arange(1000, dtype=jnp.float32)
    roots = 0.00085 ** 0.5 + (0.012 ** 0.5 - 0.00085 ** 0.5) * levels / 999.0
    signals = jnp.exp(jnp.cumsum(jnp.log1p(-roots * roots)))
    return jnp.sum(jnp.where(jnp.arange(1000) == timestep, signals, 0.0))

def time_features(timestep, channels):
    halfway = channels // 2
    freqs = jnp.exp(-math.log(10000.0) * jnp.arange(halfway, dtype=jnp.float32) / halfway)
    angles = timestep.astype(jnp.float32) * freqs
    return jnp.concatenate([jnp.cos(angles), jnp.sin(angles)])[None, :]

def group_norm(values, gain, offset, epsilon):
    pixels, channels = values.shape
    grouped = values.reshape(pixels, GROUPS, channels // GROUPS)
    average = lax.optimization_barrier(jnp.mean(grouped, axis=(0, 2), keepdims=True))
    spread = lax.optimization_barrier(jnp.mean(jnp.square(grouped - average), axis=(0, 2), keepdims=True))
    normal = ((grouped - average) * lax.rsqrt(spread + epsilon)).reshape(pixels, channels)
    return normal * gain + offset

def norm_silu(values, gain, offset, epsilon):
    return jax.nn.silu(group_norm(values, gain, offset, epsilon))

def layer_norm(values, gain, offset):
    average = lax.optimization_barrier(jnp.mean(values, axis=1, keepdims=True))
    spread = lax.optimization_barrier(jnp.mean(jnp.square(values - average), axis=1, keepdims=True))
    return (values - average) * lax.rsqrt(spread + 1e-05) * gain + offset

def geglu(gated):
    halfway = gated.shape[1] // 2
    return gated[:, :halfway] * jax.nn.gelu(gated[:, halfway:], approximate=False)

def unpack(vector_table):
    return dict(input_kernel=vector_table[0:36], output_kernel=vector_table[36:72], input_bias=vector_table[72], norm_one=vector_table[73:75], block_one_bias=vector_table[75], time_in_bias=vector_table[76:80].reshape(-1), middle_bias=vector_table[80:84].reshape(-1), time_out_bias=vector_table[84], norm_two=vector_table[85:87], block_two_bias=vector_table[87], norm_three=vector_table[88:90], project_in_bias=vector_table[90], layer_one=vector_table[91:93], self_bias=vector_table[93], layer_two=vector_table[94:96], cross_bias=vector_table[96], layer_three=vector_table[97:99], gate_bias=vector_table[99:107].reshape(-1), down_bias=vector_table[107], project_out_bias=vector_table[108], norm_out=vector_table[109:111], output_bias=vector_table[111, 0:4])

def conv_three(image, kernel):
    channels = image.shape[1]
    padded = jnp.pad(image.reshape(SIDE, SIDE, channels), ((1, 1), (1, 1), (0, 0)))
    summed = jnp.zeros((SIDE * SIDE, kernel.shape[2]), jnp.float32)
    for tap_index in range(9):
        row_offset, col_offset = (tap_index // 3, tap_index % 3)
        window = padded[row_offset:row_offset + SIDE, col_offset:col_offset + SIDE].reshape(SIDE * SIDE, channels)
        summed = summed + product(window, kernel[tap_index])
    return summed

def attention(queries, key_rows, values):
    head_query = queries.reshape(queries.shape[0], HEADS, HEAD_DIM)
    head_keys = key_rows.reshape(key_rows.shape[0], HEADS, HEAD_DIM)
    head_values = values.reshape(values.shape[0], HEADS, HEAD_DIM)
    scores = low_back(jnp.einsum('qhd,khd->hqk', head_query, head_keys, precision=highest)) * HEAD_DIM ** (-0.5)
    weights = low(jax.nn.softmax(scores, axis=2))
    attended = jnp.einsum('hqk,khd->qhd', weights, head_values, precision=highest)
    return low(low_back(attended.reshape(queries.shape[0], HEADS * HEAD_DIM)))

def forward_loss(masters, batch, mask_total):
    kernels, entry, middle, narrow, crossing, widen, vectors, squares = [low(piece) for piece in masters]
    table = unpack(vectors)
    input_kernel = table['input_kernel'].reshape(9, 4, C)
    output_kernel = table['output_kernel'].reshape(9, 4, C).transpose(0, 2, 1)
    kernel_one = kernels[0].reshape(9, C, C)
    kernel_two = kernels[1].reshape(9, C, C)
    joined_qkv = jnp.concatenate([squares[0], squares[1], squares[2]], axis=1)

    def one_sample(latent, noise, context, timestep, region):
        signal = noise_level(timestep)
        noised = low(jnp.sqrt(signal) * latent + jnp.sqrt(1.0 - signal) * noise).T
        hidden = low_back(conv_three(noised, input_kernel) + table['input_bias'])
        feature = low(time_features(timestep, C))
        first_act = low(jax.nn.silu(low_back(product(feature, entry) + table['time_in_bias'])))
        second_pre = low_back(product(first_act, middle) + table['middle_bias'])
        embedding = low_back(product(low(jax.nn.silu(second_pre)), narrow[0]) + table['time_out_bias'])
        act_one = low(norm_silu(hidden, table['norm_one'][0], table['norm_one'][1], 1e-05))
        inner_act = low_back(conv_three(act_one, kernel_one) + table['block_one_bias'] + embedding)
        act_two = low(norm_silu(inner_act, table['norm_two'][0], table['norm_two'][1], 1e-05))
        residual = hidden + low_back(conv_three(act_two, kernel_two) + table['block_two_bias'])
        normed = low(group_norm(residual, table['norm_three'][0], table['norm_three'][1], 1e-06))
        stream = low_back(product(normed, squares[6]) + table['project_in_bias'])
        lay_one = low(layer_norm(stream, table['layer_one'][0], table['layer_one'][1]))
        triple = low(low_back(product(lay_one, joined_qkv)))
        attended = attention(triple[:, :C], triple[:, C:2 * C], triple[:, 2 * C:])
        stream = stream + low_back(product(attended, squares[3]) + table['self_bias'])
        lay_two = low(layer_norm(stream, table['layer_two'][0], table['layer_two'][1]))
        cross_query = low(low_back(product(lay_two, squares[4])))
        key_value = low(low_back(product(context, crossing)))
        attended = attention(cross_query, key_value[:, :C], key_value[:, C:])
        stream = stream + low_back(product(attended, squares[5]) + table['cross_bias'])
        lay_three = low(layer_norm(stream, table['layer_three'][0], table['layer_three'][1]))
        gated = low_back(product(lay_three, widen) + table['gate_bias'])
        stream = stream + low_back(product(low(geglu(gated)), narrow[1]) + table['down_bias'])
        residual = residual + low_back(product(low(stream), squares[7]) + table['project_out_bias'])
        act_out = low(norm_silu(residual, table['norm_out'][0], table['norm_out'][1], 1e-05))
        output = low_back(conv_three(act_out, output_kernel) + table['output_bias'])
        ratio = signal / (1.0 - signal)
        factor = jnp.minimum(ratio, 5.0) / ratio
        mismatch = output.T - noise
        return factor * jnp.sum(region * mismatch * mismatch) / (4.0 * mask_total)

    def scan_step(summed, sample):
        return (summed + jax.checkpoint(one_sample)(*sample), None)
    summed, unused = lax.scan(scan_step, jnp.zeros((), jnp.float32), batch)
    return summed

def adam(weight, first, second, gradient, rate, fix_one, fix_two):
    moment = beta_one * first + (1.0 - beta_one) * gradient
    variance = beta_two * second + (1.0 - beta_two) * gradient * gradient
    update = moment / fix_one / (jnp.sqrt(variance / fix_two) + adam_eps)
    return (weight - rate * (update + decay * weight), moment, variance)

def turned(left_basis, matrix, right_basis):
    return jnp.matmul(jnp.matmul(jnp.swapaxes(left_basis, 1, 2), matrix, precision=highest), right_basis, precision=highest)

def orthonormal(matrix):
    gram_matrix = jnp.matmul(jnp.swapaxes(matrix, 1, 2), matrix, precision=highest)
    cholesky_factor = jnp.linalg.cholesky(gram_matrix)
    solved = jax.scipy.linalg.solve_triangular(cholesky_factor, jnp.swapaxes(matrix, 1, 2), lower=True)
    return jnp.swapaxes(solved, 1, 2)

def soap_step(gradient, state, fix_one, fix_two):
    moment = beta_one * state[0] + (1.0 - beta_one) * gradient
    rotated = turned(state[4], gradient, state[5])
    second = beta_two * state[1] + (1.0 - beta_two) * rotated * rotated
    scaled = turned(state[4], moment, state[5]) / fix_one / (jnp.sqrt(second / fix_two) + adam_eps)
    direction = jnp.matmul(jnp.matmul(state[4], scaled, precision=highest), jnp.swapaxes(state[5], 1, 2), precision=highest)
    left_stat = beta_stat * state[2] + (1.0 - beta_stat) * jnp.matmul(gradient, jnp.swapaxes(gradient, 1, 2), precision=highest)
    right_stat = beta_stat * state[3] + (1.0 - beta_stat) * jnp.matmul(jnp.swapaxes(gradient, 1, 2), gradient, precision=highest)
    basis_left = orthonormal(jnp.matmul(left_stat, state[4], precision=highest))
    basis_right = orthonormal(jnp.matmul(right_stat, state[5], precision=highest))
    return (direction, jnp.stack([basis_left, basis_right]))

def reference(latents, noise, context, timesteps, region_mask, owners, step_count, kernels_weight, kernels_first, kernels_second, entry_weight, entry_first, entry_second, middle_weight, middle_first, middle_second, narrow_weight, narrow_first, narrow_second, crossing_weight, crossing_first, crossing_second, widen_weight, widen_first, widen_second, vectors_weight, vectors_first, vectors_second, squares_weight, squares_state):
    mask_total = jnp.sum(region_mask.astype(jnp.float32))
    every = MICRO * SAMPLES
    batch = (latents.astype(jnp.float32).reshape(every, 4, TOK), noise.astype(jnp.float32).reshape(every, 4, TOK), context.astype(jnp.float32).reshape(every, CTX_LEN, CTX_DIM), timesteps.reshape(every), region_mask.astype(jnp.float32).reshape(every, TOK))
    masters = (kernels_weight, entry_weight, middle_weight, narrow_weight, crossing_weight, widen_weight, vectors_weight, squares_weight)
    loss, pullback = jax.vjp(lambda *weights: forward_loss(weights, batch, mask_total), *masters)
    raw_grads = pullback(jnp.ones((), jnp.float32))
    grad_norm = jnp.sqrt(sum((jnp.sum(piece * piece) for piece in raw_grads)))
    clip = jnp.minimum(1.0, clip_limit / grad_norm)
    grads = [piece * clip for piece in raw_grads]
    steps = step_count[0].astype(jnp.float32)
    fix_one = 1.0 - jnp.power(jnp.float32(beta_one), steps)
    fix_two = 1.0 - jnp.power(jnp.float32(beta_two), steps)
    rate_list = rates()
    kernels_master, kernels_moment, kernels_variance = adam(kernels_weight, kernels_first, kernels_second, grads[0], rate_list[0], fix_one, fix_two)
    entry_master, entry_moment, entry_variance = adam(entry_weight, entry_first, entry_second, grads[1], rate_list[1], fix_one, fix_two)
    middle_master, middle_moment, middle_variance = adam(middle_weight, middle_first, middle_second, grads[2], rate_list[2], fix_one, fix_two)
    narrow_master, narrow_moment, narrow_variance = adam(narrow_weight, narrow_first, narrow_second, grads[3], rate_list[3], fix_one, fix_two)
    crossing_master, crossing_moment, crossing_variance = adam(crossing_weight, crossing_first, crossing_second, grads[4], rate_list[4], fix_one, fix_two)
    widen_master, widen_moment, widen_variance = adam(widen_weight, widen_first, widen_second, grads[5], rate_list[5], fix_one, fix_two)
    vectors_master, vectors_moment, vectors_variance = adam(vectors_weight, vectors_first, vectors_second, grads[6], rate_list[6], fix_one, fix_two)
    squares_grad = grads[7][owners]
    direction, squares_slots = soap_step(squares_grad, squares_state, fix_one, fix_two)
    full_direction = jnp.zeros_like(squares_weight).at[owners].set(direction)
    squares_master = squares_weight - rate_list[7] * (full_direction + decay * squares_weight)
    totals = jnp.stack([loss, grad_norm])
    return (totals, kernels_master, kernels_moment, kernels_variance, entry_master, entry_moment, entry_variance, middle_master, middle_moment, middle_variance, narrow_master, narrow_moment, narrow_variance, crossing_master, crossing_moment, crossing_variance, widen_master, widen_moment, widen_variance, vectors_master, vectors_moment, vectors_variance, squares_master, squares_slots, squares_grad)
```

```python
from functools import partial
import math

import jax
import jax.numpy as jnp
from jax import lax
from jax.experimental import pallas as pl
from jax.experimental.pallas import tpu as pltpu
from jax.sharding import PartitionSpec as P

C = 320
HEADS = 8
GROUPS = 32
CTX_DIM = 768
SIDE = 32
HEAD_DIM = 40


highest = lax.Precision.HIGHEST
beta_one = 0.9
beta_two = 0.999
beta_stat = 0.95
adam_eps = 1e-08
decay = 0.01
clip_limit = 0.002


def lowered(values):
    return values.astype(jnp.bfloat16)


def product(left_matrix, right_matrix):
    return jnp.dot(left_matrix, right_matrix, preferred_element_type=jnp.float32)


def product_left(left_matrix, right_matrix):
    return lax.dot_general(
        left_matrix, right_matrix, (((0,), (0,)), ((), ())), preferred_element_type=jnp.float32
    )


def product_right(left_matrix, right_matrix):
    return lax.dot_general(
        left_matrix, right_matrix, (((1,), (1,)), ((), ())), preferred_element_type=jnp.float32
    )


def column_sum(values):
    return jnp.sum(values.astype(jnp.float32), axis=0)


def rates():
    return (
        3.0 / math.sqrt(9 * C),
        3.0 / math.sqrt(C),
        3.0 / math.sqrt(4 * C),
        3.0 / math.sqrt(4 * C),
        3.0 / math.sqrt(CTX_DIM),
        3.0 / math.sqrt(C),
        0.3,
        3.0 / math.sqrt(C),
    )


def noise_level(timestep):
    levels = jnp.arange(1000, dtype=jnp.float32)
    roots = 0.00085**0.5 + (0.012**0.5 - 0.00085**0.5) * levels / 999.0
    signals = jnp.exp(jnp.cumsum(jnp.log1p(-roots * roots)))
    return jnp.sum(jnp.where(jnp.arange(1000) == timestep, signals, 0.0))


def time_features(timestep, channels):
    halfway = channels // 2
    freqs = jnp.exp(-math.log(10000.0) * jnp.arange(halfway, dtype=jnp.float32) / halfway)
    angles = timestep.astype(jnp.float32) * freqs
    return jnp.concatenate([jnp.cos(angles), jnp.sin(angles)])[None, :]


def unpack(vector_table):
    return dict(
        input_bias=vector_table[72],
        norm_one=vector_table[73:75],
        block_one_bias=vector_table[75],
        time_in_bias=vector_table[76:80].reshape(-1),
        middle_bias=vector_table[80:84].reshape(-1),
        time_out_bias=vector_table[84],
        norm_two=vector_table[85:87],
        block_two_bias=vector_table[87],
        norm_three=vector_table[88:90],
        project_in_bias=vector_table[90],
        layer_one=vector_table[91:93],
        self_bias=vector_table[93],
        layer_two=vector_table[94:96],
        cross_bias=vector_table[96],
        layer_three=vector_table[97:99],
        gate_bias=vector_table[99:107].reshape(-1),
        down_bias=vector_table[107],
        project_out_bias=vector_table[108],
        norm_out=vector_table[109:111],
        output_bias=vector_table[111, 0:4],
    )


GROUP = 10
WIDE = 384
LANES = 128
QUERY_BLOCK = 256
LOG2E = 1.4426950408889634


def wide_columns(matrix):
    lead = matrix.shape[0]
    parts = []
    for start, stop in ((0, 120), (120, 240), (240, 320)):
        parts.append(
            jnp.pad(matrix[:, start:stop], ((0, 0), (0, LANES - (stop - start))))
        )
    return jnp.concatenate(parts, axis=1).reshape(lead, WIDE)


def wide_rows(matrix):
    parts = []
    for start, stop in ((0, 120), (120, 240), (240, 320)):
        parts.append(jnp.pad(matrix[start:stop], ((0, LANES - (stop - start)), (0, 0))))
    return jnp.concatenate(parts, axis=0)


def slim_columns(matrix):
    return jnp.concatenate(
        [matrix[:, 0:120], matrix[:, 128:248], matrix[:, 256:336]], axis=1
    )


def slim_rows(matrix):
    return jnp.concatenate([matrix[0:120], matrix[128:248], matrix[256:336]], axis=0)


def dot_nt(left_matrix, right_matrix):
    return lax.dot_general(
        left_matrix, right_matrix, (((1,), (1,)), ((), ())), preferred_element_type=jnp.float32
    )


def dot_nn(left_matrix, right_matrix):
    return lax.dot_general(
        left_matrix, right_matrix, (((1,), (0,)), ((), ())), preferred_element_type=jnp.float32
    )


def attend_kernel(valid, q_ref, k_ref, vt_ref, out_ref, total_ref):
    tile = pl.program_id(1)
    member = pl.program_id(3)
    scaling = HEAD_DIM ** (-0.5) * LOG2E

    @pl.when(tile * 3 + member < HEADS)
    def _():
        low_lane = member * HEAD_DIM
        lane = lax.broadcasted_iota(jnp.int32, (QUERY_BLOCK, LANES), 1)
        chosen = (lane >= low_lane) & (lane < low_lane + HEAD_DIM)
        query = jnp.where(chosen, q_ref[...], jnp.zeros((), jnp.bfloat16))
        scores = dot_nt(k_ref[...], query)
        if valid < scores.shape[0]:
            row = lax.broadcasted_iota(jnp.int32, scores.shape, 0)
            scores = jnp.where(row < valid, scores, -1e30)
        maximum = jnp.max(scores, axis=0, keepdims=True) * scaling
        exponent = jnp.exp2(scores * scaling - maximum)
        summed = jnp.sum(exponent, axis=0, keepdims=True)
        weights = (exponent * (1.0 / summed)).astype(jnp.bfloat16)
        attended = dot_nn(vt_ref[...], weights)
        row = lax.broadcasted_iota(jnp.int32, attended.shape, 0)
        inside = (row >= low_lane) & (row < low_lane + HEAD_DIM)
        earlier = jnp.where(member == 0, 0.0, out_ref[...].astype(jnp.float32))
        out_ref[...] = jnp.where(inside, attended, earlier).astype(jnp.bfloat16)
        total_ref[pl.ds(member, 1), :] = maximum + jnp.log2(summed)


def attend(queries, key_rows, values_turned, valid):
    samples, pixels, wide = queries.shape
    keys = key_rows.shape[1]
    blocks = pixels // QUERY_BLOCK
    return pl.pallas_call(
        partial(attend_kernel, valid),
        grid=(samples, wide // LANES, blocks, 3),
        in_specs=[
            pl.BlockSpec((None, QUERY_BLOCK, LANES), lambda s, t, b, j: (s, b, t)),
            pl.BlockSpec((None, keys, LANES), lambda s, t, b, j: (s, 0, t)),
            pl.BlockSpec((None, LANES, keys), lambda s, t, b, j: (s, t, 0)),
        ],
        out_specs=[
            pl.BlockSpec((None, LANES, QUERY_BLOCK), lambda s, t, b, j: (s, t, b)),
            pl.BlockSpec((None, None, 8, QUERY_BLOCK), lambda s, t, b, j: (s, t, 0, b)),
        ],
        out_shape=[
            jax.ShapeDtypeStruct((samples, wide, pixels), jnp.bfloat16),
            jax.ShapeDtypeStruct((samples, wide // LANES, 8, pixels), jnp.float32),
        ],
        compiler_params=pltpu.CompilerParams(vmem_limit_bytes=24 * 1024 * 1024),
        cost_estimate=pl.CostEstimate(
            flops=samples * HEADS * pixels * keys * 512,
            bytes_accessed=samples * pixels * wide * 8,
            transcendentals=samples * HEADS * pixels * keys,
        ),
        name="attend",
    )(queries, key_rows, values_turned)


def attend_back_kernel(
    valid,
    q_ref,
    k_ref,
    kt_ref,
    v_ref,
    delta_ref,
    total_ref,
    dq_ref,
    dk_ref,
    dv_ref,
    dk_sum,
    dv_sum,
):
    tile = pl.program_id(1)
    block = pl.program_id(2)
    member = pl.program_id(3)
    scaling = HEAD_DIM ** (-0.5) * LOG2E

    @pl.when((block == 0) & (member == 0))
    def _():
        dk_sum[...] = jnp.zeros_like(dk_sum)
        dv_sum[...] = jnp.zeros_like(dv_sum)

    @pl.when(tile * 3 + member < HEADS)
    def _():
        low_lane = member * HEAD_DIM
        lane = lax.broadcasted_iota(jnp.int32, (QUERY_BLOCK, LANES), 1)
        chosen = (lane >= low_lane) & (lane < low_lane + HEAD_DIM)
        query = jnp.where(chosen, q_ref[...], jnp.zeros((), jnp.bfloat16))
        row = lax.broadcasted_iota(jnp.int32, (LANES, QUERY_BLOCK), 0)
        inside = (row >= low_lane) & (row < low_lane + HEAD_DIM)
        delta = jnp.where(inside, delta_ref[...], jnp.zeros((), jnp.bfloat16))
        scores = dot_nt(k_ref[...], query)
        weights = jnp.exp2(scores * scaling - total_ref[pl.ds(member, 1), :])
        if valid < scores.shape[0]:
            key_row = lax.broadcasted_iota(jnp.int32, scores.shape, 0)
            weights = jnp.where(key_row < valid, weights, 0.0)
        delta_weights = dot_nn(v_ref[...], delta)
        dv_sum[...] += dot_nt(weights.astype(jnp.bfloat16), delta)
        middle = jnp.sum(delta_weights * weights, axis=0, keepdims=True)
        coarse = (weights * (delta_weights - middle) * HEAD_DIM ** (-0.5)).astype(jnp.bfloat16)
        dk_sum[...] += dot_nn(coarse, query)
        delta_query = dot_nn(kt_ref[...], coarse)
        earlier = jnp.where(member == 0, 0.0, dq_ref[...].astype(jnp.float32))
        dq_ref[...] = jnp.where(inside, delta_query, earlier).astype(jnp.bfloat16)

    @pl.when((block == pl.num_programs(2) - 1) & (member == 2))
    def _():
        dk_ref[...] = dk_sum[...].astype(jnp.bfloat16)
        dv_ref[...] = dv_sum[...].astype(jnp.bfloat16)


def attend_back(queries, key_rows, keys_turned, values, delta_turned, totals, valid):
    samples, pixels, wide = queries.shape
    keys = key_rows.shape[1]
    blocks = pixels // QUERY_BLOCK
    key_spec = pl.BlockSpec((None, keys, LANES), lambda s, t, b, j: (s, 0, t))
    turned_spec = pl.BlockSpec((None, LANES, QUERY_BLOCK), lambda s, t, b, j: (s, t, b))
    return pl.pallas_call(
        partial(attend_back_kernel, valid),
        grid=(samples, wide // LANES, blocks, 3),
        in_specs=[
            pl.BlockSpec((None, QUERY_BLOCK, LANES), lambda s, t, b, j: (s, b, t)),
            key_spec,
            pl.BlockSpec((None, LANES, keys), lambda s, t, b, j: (s, t, 0)),
            key_spec,
            turned_spec,
            pl.BlockSpec((None, None, 8, QUERY_BLOCK), lambda s, t, b, j: (s, t, 0, b)),
        ],
        out_specs=[turned_spec, key_spec, key_spec],
        out_shape=[
            jax.ShapeDtypeStruct((samples, wide, pixels), jnp.bfloat16),
            jax.ShapeDtypeStruct((samples, keys, wide), jnp.bfloat16),
            jax.ShapeDtypeStruct((samples, keys, wide), jnp.bfloat16),
        ],
        scratch_shapes=[pltpu.VMEM((keys, LANES), jnp.float32)] * 2,
        compiler_params=pltpu.CompilerParams(vmem_limit_bytes=24 * 1024 * 1024),
        cost_estimate=pl.CostEstimate(
            flops=samples * HEADS * pixels * keys * 1280,
            bytes_accessed=samples * pixels * wide * 16,
            transcendentals=samples * HEADS * pixels * keys,
        ),
        name="attend_back",
    )(queries, key_rows, keys_turned, values, delta_turned, totals)


def group_spread(sums, count):
    channels = sums.shape[-1]
    index = jnp.arange(channels) // GROUP
    mixer = (index[:, None] == index[None, :]).astype(jnp.float32)
    return jnp.matmul(sums, mixer, precision=highest) / count


def group_stats(values, epsilon):
    count = values.shape[1] * GROUP
    average = group_spread(jnp.sum(values, axis=1), count)[:, None, :]
    spread = group_spread(jnp.sum(jnp.square(values - average), axis=1), count)[:, None, :]
    return average, lax.rsqrt(spread + epsilon)


def group_apply(values, stats, gains):
    return (values - stats[0]) * stats[1] * gains[0] + gains[1]


def group_back(values, stats, gains, delta):
    count = values.shape[1] * GROUP
    normal = (values - stats[0]) * stats[1]
    offset_sum = jnp.sum(delta, axis=1)
    gain_sum = jnp.sum(delta * normal, axis=1)
    first = group_spread(offset_sum * gains[0], count)[:, None, :]
    second = group_spread(gain_sum * gains[0], count)[:, None, :]
    result = stats[1] * (delta * gains[0] - first - normal * second)
    return result, jnp.sum(gain_sum, axis=0), jnp.sum(offset_sum, axis=0)


def silu_slope(values, delta):
    gate = jax.nn.sigmoid(values)
    return delta * gate * (1.0 + values * (1.0 - gate))


def layer_norm(values, gains):
    average = jnp.mean(values, axis=-1, keepdims=True)
    spread = jnp.mean(jnp.square(values - average), axis=-1, keepdims=True)
    return (values - average) * lax.rsqrt(spread + 1e-05) * gains[0] + gains[1]


def layer_back(values, gains, delta):
    average = jnp.mean(values, axis=-1, keepdims=True)
    spread = jnp.mean(jnp.square(values - average), axis=-1, keepdims=True)
    scale = lax.rsqrt(spread + 1e-05)
    normal = (values - average) * scale
    scaled = delta * gains[0]
    result = scale * (
        scaled
        - jnp.mean(scaled, axis=-1, keepdims=True)
        - normal * jnp.mean(scaled * normal, axis=-1, keepdims=True)
    )
    return (
        result,
        jnp.sum(delta * normal, axis=(0, 1)),
        jnp.sum(delta, axis=(0, 1)),
    )


def conv(image, kernel):
    samples = image.shape[0]
    result = lax.conv_general_dilated(
        image.reshape(samples, SIDE, SIDE, -1),
        kernel.reshape(3, 3, C, C),
        (1, 1),
        ((1, 1), (1, 1)),
        dimension_numbers=("NHWC", "HWIO", "NHWC"),
        preferred_element_type=jnp.float32,
    )
    return result.reshape(samples, SIDE * SIDE, C)


def conv_back(delta, kernel):
    samples = delta.shape[0]
    result = lax.conv_general_dilated(
        delta.reshape(samples, SIDE, SIDE, -1),
        kernel.reshape(3, 3, C, C)[::-1, ::-1],
        (1, 1),
        ((1, 1), (1, 1)),
        dimension_numbers=("NHWC", "HWOI", "NHWC"),
        preferred_element_type=jnp.float32,
    )
    return result.reshape(samples, SIDE * SIDE, C)


def conv_gradient(image, delta):
    samples = image.shape[0]
    result = lax.conv_general_dilated(
        image.reshape(samples, SIDE, SIDE, -1),
        delta.reshape(samples, SIDE, SIDE, -1),
        (1, 1),
        ((1, 1), (1, 1)),
        dimension_numbers=("CHWN", "IHWO", "HWNC"),
        preferred_element_type=jnp.float32,
    )
    return result.reshape(9 * C, C)


def shifted_taps(image, sign):
    pixels = image.shape[-1]
    edge = SIDE + 1
    column = jnp.arange(pixels) % SIDE
    padded = jnp.pad(image, ((0, 0), (0, 0), (edge, edge)))
    pieces = []
    for tap in range(9):
        down, across = sign * (tap // 3 - 1), sign * (tap % 3 - 1)
        start = edge + SIDE * down + across
        piece = padded[:, :, start : start + pixels]
        if across == -1:
            piece = jnp.where(column >= 1, piece, jnp.zeros((), piece.dtype))
        if across == 1:
            piece = jnp.where(column < SIDE - 1, piece, jnp.zeros((), piece.dtype))
        pieces.append(piece)
    return pieces


def rows_dot(left, right):
    return lax.dot_general(
        left, right, (((0, 1), (0, 1)), ((), ())), preferred_element_type=jnp.float32
    )


def times(left, right):
    return lax.dot_general(
        left, right, (((2,), (0,)), ((), ())), preferred_element_type=jnp.float32
    )


def times_back(left, right):
    return lax.dot_general(
        left, right, (((2,), (1,)), ((), ())), preferred_element_type=jnp.float32
    )


def turned_times(left, right):
    return jnp.einsum("sdp,dc->spc", left, right, preferred_element_type=jnp.float32)


def turned_product(values, matrix):
    return jnp.einsum("spc,cd->sdp", values, matrix, preferred_element_type=jnp.float32)


def rows_total(values):
    return jnp.sum(values.astype(jnp.float32), axis=(0, 1))


def device_pass(weights, latents, noise, context, timesteps, region, mask_total):
    kernels, entry, middle, narrow, vectors, squares, crossing, widen = weights
    table = unpack(vectors.astype(jnp.float32))
    samples, channels_in, pixels = latents.shape
    words = context.shape[1]
    word_rows = -(-words // 16) * 16
    signal = jax.vmap(noise_level)(timesteps)[:, None, None]
    noise_value = noise.astype(jnp.float32)
    noised = lowered(
        jnp.sqrt(signal) * latents.astype(jnp.float32) + jnp.sqrt(1.0 - signal) * noise_value
    )
    columns_in = jnp.concatenate(shifted_taps(noised, 1), axis=1)
    hidden = turned_times(columns_in, vectors[0:36]) + table["input_bias"]
    feature = lowered(jax.vmap(lambda t: time_features(t, C)[0])(timesteps))
    first_pre = product(feature, entry) + table["time_in_bias"]
    first_low = lowered(jax.nn.silu(first_pre))
    second_pre = product(first_low, middle) + table["middle_bias"]
    second_low = lowered(jax.nn.silu(second_pre))
    embedding = product(second_low, narrow[0]) + table["time_out_bias"]
    stats_one = group_stats(hidden, 1e-05)
    act_one = lowered(jax.nn.silu(group_apply(hidden, stats_one, table["norm_one"])))
    inner_act = conv(act_one, kernels[0]) + table["block_one_bias"] + embedding[:, None, :]
    stats_two = group_stats(inner_act, 1e-05)
    act_two = lowered(jax.nn.silu(group_apply(inner_act, stats_two, table["norm_two"])))
    residual = hidden + conv(act_two, kernels[1]) + table["block_two_bias"]
    stats_three = group_stats(residual, 1e-06)
    normed = lowered(group_apply(residual, stats_three, table["norm_three"]))
    stream = times(normed, squares[6]) + table["project_in_bias"]
    lay_one = lowered(layer_norm(stream, table["layer_one"]))
    wide_query, wide_key, wide_value = (wide_columns(squares[index]) for index in range(3))
    queries = lowered(times(lay_one, wide_query))
    keys = lowered(times(lay_one, wide_key))
    values = lowered(times(lay_one, wide_value))
    attended, totals = attend(queries, keys, jnp.swapaxes(values, 1, 2), pixels)
    wide_self = wide_rows(squares[3])
    stream_two = stream + turned_times(attended, wide_self) + table["self_bias"]
    lay_two = lowered(layer_norm(stream_two, table["layer_two"]))
    wide_cross_query = wide_columns(squares[4])
    cross_query = lowered(times(lay_two, wide_cross_query))
    wide_context = jnp.pad(context, ((0, 0), (0, word_rows - words), (0, 0)))
    cross_key = lowered(times(wide_context, wide_columns(crossing[:, :C])))
    cross_value = lowered(times(wide_context, wide_columns(crossing[:, C:])))
    cross_attended, cross_totals = attend(
        cross_query, cross_key, jnp.swapaxes(cross_value, 1, 2), words
    )
    wide_cross = wide_rows(squares[5])
    stream_three = stream_two + turned_times(cross_attended, wide_cross) + table["cross_bias"]
    lay_three = lowered(layer_norm(stream_three, table["layer_three"]))
    gated = times(lay_three, widen) + table["gate_bias"]
    halfway = gated.shape[-1] // 2
    gated_low = lowered(
        gated[..., :halfway] * jax.nn.gelu(gated[..., halfway:], approximate=False)
    )
    stream_low = lowered(stream_three + times(gated_low, narrow[1]) + table["down_bias"])
    residual_two = residual + times(stream_low, squares[7]) + table["project_out_bias"]
    stats_out = group_stats(residual_two, 1e-05)
    act_out = lowered(jax.nn.silu(group_apply(residual_two, stats_out, table["norm_out"])))
    output_kernel = vectors[36:72]
    tap_outputs = jnp.einsum(
        "kc,spc->skp", output_kernel, act_out, preferred_element_type=jnp.float32
    )
    output = table["output_bias"][None, :, None] + sum(
        shifted_taps(tap_outputs[:, 4 * tap : 4 * tap + 4], 1)[tap] for tap in range(9)
    )
    ratio = signal / (1.0 - signal)
    factor = jnp.minimum(ratio, 5.0) / ratio
    mismatch = output - noise_value
    region_value = region.astype(jnp.float32)[:, None, :]
    loss = jnp.sum(factor * region_value * mismatch * mismatch) / (4.0 * mask_total)

    coarse_output = lowered(factor * 2.0 / (4.0 * mask_total) * region_value * mismatch)
    output_columns = jnp.concatenate(shifted_taps(coarse_output, -1), axis=1)
    output_rows = jnp.einsum(
        "skp,spc->kc", output_columns, act_out, preferred_element_type=jnp.float32
    )
    delta = turned_times(output_columns, output_kernel)
    delta = silu_slope(group_apply(residual_two, stats_out, table["norm_out"]), delta)
    delta_two, out_gain, out_offset = group_back(
        residual_two, stats_out, table["norm_out"], delta
    )
    coarse_project = lowered(delta_two)
    project_out_gradient = rows_dot(stream_low, coarse_project)
    delta_stream = times_back(coarse_project, squares[7])
    coarse_down = lowered(delta_stream)
    down_gradient = rows_dot(gated_low, coarse_down)
    delta_gated = times_back(coarse_down, narrow[1])
    gate_values = gated[..., halfway:]
    normal_cdf = 0.5 * (1.0 + lax.erf(gate_values * math.sqrt(0.5)))
    normal_pdf = jnp.exp(-0.5 * gate_values * gate_values) * (1.0 / math.sqrt(2.0 * math.pi))
    coarse_gated = lowered(
        jnp.concatenate(
            [
                delta_gated * gate_values * normal_cdf,
                delta_gated * gated[..., :halfway] * (normal_cdf + gate_values * normal_pdf),
            ],
            axis=-1,
        )
    )
    widen_gradient = rows_dot(lay_three, coarse_gated)
    delta_part, three_gain, three_offset = layer_back(
        stream_three, table["layer_three"], times_back(coarse_gated, widen)
    )
    delta_stream = delta_stream + delta_part
    coarse_cross = lowered(delta_stream)
    cross_out_gradient = slim_rows(
        jnp.einsum("sdp,spc->dc", cross_attended, coarse_cross, preferred_element_type=jnp.float32)
    )
    coarse_attended = lowered(
        jnp.einsum("dc,spc->sdp", wide_cross, coarse_cross, preferred_element_type=jnp.float32)
    )
    delta_query, delta_key, delta_value = attend_back(
        cross_query,
        cross_key,
        jnp.swapaxes(cross_key, 1, 2),
        cross_value,
        coarse_attended,
        cross_totals,
        words,
    )
    cross_query_gradient = slim_columns(
        jnp.einsum("spc,sdp->cd", lay_two, delta_query, preferred_element_type=jnp.float32)
    )
    crossing_gradient = jnp.concatenate(
        [
            slim_columns(rows_dot(wide_context, delta_key)),
            slim_columns(rows_dot(wide_context, delta_value)),
        ],
        axis=1,
    )
    delta_part, two_gain, two_offset = layer_back(
        stream_two,
        table["layer_two"],
        jnp.einsum("sdp,cd->spc", delta_query, wide_cross_query, preferred_element_type=jnp.float32),
    )
    delta_stream = delta_stream + delta_part
    coarse_self = lowered(delta_stream)
    self_out_gradient = slim_rows(
        jnp.einsum("sdp,spc->dc", attended, coarse_self, preferred_element_type=jnp.float32)
    )
    coarse_attended = lowered(
        jnp.einsum("dc,spc->sdp", wide_self, coarse_self, preferred_element_type=jnp.float32)
    )
    delta_query, delta_key, delta_value = attend_back(
        queries, keys, jnp.swapaxes(keys, 1, 2), values, coarse_attended, totals, pixels
    )
    query_gradient = slim_columns(
        jnp.einsum("spc,sdp->cd", lay_one, delta_query, preferred_element_type=jnp.float32)
    )
    key_gradient = slim_columns(rows_dot(lay_one, delta_key))
    value_gradient = slim_columns(rows_dot(lay_one, delta_value))
    delta_lay = (
        jnp.einsum("sdp,cd->spc", delta_query, wide_query, preferred_element_type=jnp.float32)
        + times_back(delta_key, wide_key)
        + times_back(delta_value, wide_value)
    )
    delta_part, one_gain, one_offset = layer_back(stream, table["layer_one"], delta_lay)
    coarse_stream = lowered(delta_stream + delta_part)
    project_in_gradient = rows_dot(normed, coarse_stream)
    delta_part, norm_three_gain, norm_three_offset = group_back(
        residual, stats_three, table["norm_three"], times_back(coarse_stream, squares[6])
    )
    delta_residual = delta_two + delta_part
    coarse_block_two = lowered(delta_residual)
    kernel_two_gradient = conv_gradient(act_two, coarse_block_two)
    delta = silu_slope(
        group_apply(inner_act, stats_two, table["norm_two"]),
        conv_back(coarse_block_two, kernels[1]),
    )
    delta_inner, norm_two_gain, norm_two_offset = group_back(
        inner_act, stats_two, table["norm_two"], delta
    )
    coarse_inner = lowered(delta_inner)
    kernel_one_gradient = conv_gradient(act_one, coarse_inner)
    delta = silu_slope(
        group_apply(hidden, stats_one, table["norm_one"]), conv_back(coarse_inner, kernels[0])
    )
    delta_part, norm_one_gain, norm_one_offset = group_back(
        hidden, stats_one, table["norm_one"], delta
    )
    coarse_hidden = lowered(delta_residual + delta_part)
    input_rows = jnp.einsum(
        "skp,spc->kc", columns_in, coarse_hidden, preferred_element_type=jnp.float32
    )
    inner_total = jnp.sum(coarse_inner.astype(jnp.float32), axis=1)
    coarse_embedding = lowered(inner_total)
    coarse_second = lowered(silu_slope(second_pre, product_right(coarse_embedding, narrow[0])))
    coarse_first = lowered(silu_slope(first_pre, product_right(coarse_second, middle)))
    bias_row = jnp.pad(
        jnp.sum(coarse_output.astype(jnp.float32), axis=(0, 2)), (0, C - channels_in)
    )
    pieces = [
        input_rows,
        output_rows,
        rows_total(coarse_hidden),
        norm_one_gain,
        norm_one_offset,
        jnp.sum(inner_total, axis=0),
        column_sum(coarse_first),
        column_sum(coarse_second),
        column_sum(coarse_embedding),
        norm_two_gain,
        norm_two_offset,
        rows_total(coarse_block_two),
        norm_three_gain,
        norm_three_offset,
        rows_total(coarse_stream),
        one_gain,
        one_offset,
        rows_total(coarse_self),
        two_gain,
        two_offset,
        rows_total(coarse_cross),
        three_gain,
        three_offset,
        rows_total(coarse_gated),
        rows_total(coarse_down),
        rows_total(coarse_project),
        out_gain,
        out_offset,
        bias_row,
    ]
    vectors_gradient = jnp.concatenate([piece.reshape(-1, C) for piece in pieces], axis=0)
    squares_gradient = [
        query_gradient,
        key_gradient,
        value_gradient,
        self_out_gradient,
        cross_query_gradient,
        cross_out_gradient,
        project_in_gradient,
        project_out_gradient,
    ]
    factors = jnp.concatenate([feature, first_low, second_low], axis=1)
    deltas = jnp.concatenate([coarse_first, coarse_second, coarse_embedding], axis=1)
    return (
        loss,
        (kernel_one_gradient, kernel_two_gradient),
        down_gradient,
        crossing_gradient,
        widen_gradient,
        vectors_gradient,
        squares_gradient,
        factors,
        deltas,
    )


def adam(weight, first, second, gradient, rate, fix_one, fix_two):
    moment = beta_one * first + (1.0 - beta_one) * gradient
    variance = beta_two * second + (1.0 - beta_two) * gradient * gradient
    update = moment / fix_one / (jnp.sqrt(variance / fix_two) + adam_eps)
    return (weight - rate * (update + decay * weight), moment, variance)


def bit_count(size):
    return max(size.bit_length() - 1, 0)


def partner_of(position, bit):
    own = (position // (2**bit)) % 2
    return own, position + (1 - 2 * own) * (2**bit)


def greet(row_index, column_index, row_bits, column_parts):
    barrier = pltpu.get_barrier_semaphore()
    for bit in range(row_bits):
        other = partner_of(row_index, bit)[1]
        pl.semaphore_signal(
            barrier, inc=1, device_id=(other, column_index), device_id_type=pl.DeviceIdType.MESH
        )
    for step in range(1, column_parts):
        other = lax.rem(column_index + step, column_parts)
        pl.semaphore_signal(
            barrier, inc=1, device_id=(row_index, other), device_id_type=pl.DeviceIdType.MESH
        )
    pl.semaphore_wait(barrier, row_bits + column_parts - 1)


def remote(source, target, send_sem, recv_sem, device):
    return pltpu.make_async_remote_copy(
        src_ref=source,
        dst_ref=target,
        send_sem=send_sem,
        recv_sem=recv_sem,
        device_id=device,
        device_id_type=pl.DeviceIdType.MESH,
    )


def add_tiles(target, own, arrived):
    lead = target.shape[:-2]
    total = math.prod(lead)

    def one(index, carry):
        coords = []
        for extent in reversed(lead):
            coords.append(lax.rem(index, extent))
            index = index // extent
        coords = tuple(reversed(coords))
        summed = own[coords].astype(jnp.float32) + arrived[coords].astype(jnp.float32)
        target[coords] = summed.astype(target.dtype)
        return carry

    if total == 1:
        zeros = (0,) * len(lead)
        summed = own[zeros].astype(jnp.float32) + arrived[zeros].astype(jnp.float32)
        target[zeros] = summed.astype(target.dtype)
    else:
        lax.fori_loop(0, total, one, 0)


def reduce_kernel(plan, row_bits, column_parts, *refs):
    count = len(plan)
    owners_ref = refs[0]
    inputs = refs[1 : count + 1]
    factor_in = refs[count + 1]
    outputs = refs[count + 2 : 2 * count + 2]
    factor_out = refs[2 * count + 2]
    scratch = list(refs[2 * count + 3 :])
    factor_send, factor_recv = scratch.pop(), scratch.pop()
    send_sems, recv_sems = scratch.pop(), scratch.pop()
    arrived, summed, outgoing, incoming = [], [], [], []
    for _ in plan:
        arrived.append([scratch.pop(0) for _ in range(row_bits)])
        summed.append([scratch.pop(0) for _ in range(row_bits)])
        outgoing.append(scratch.pop(0))
        incoming.append(scratch.pop(0))
    row_index = lax.axis_index("dp")
    column_index = lax.axis_index("fsdp")
    orders = [
        list(range(row_bits)) if forward else [0] + list(range(row_bits - 1, 0, -1))
        for _, forward in plan
    ]
    every = slice(None)

    def halves(array, stage):
        order = orders[array]
        remaining = [bit for bit in range(row_bits - 1, -1, -1) if bit not in order[:stage]]
        source = inputs[array] if stage == 0 else summed[array][stage - 1]
        axis = plan[array][0] + remaining.index(order[stage])
        own, other = partner_of(row_index, order[stage])
        kept = source.at[(every,) * axis + (own,)]
        given = source.at[(every,) * axis + (1 - own,)]
        return kept, given, other

    def swap(array, stage):
        given, other = halves(array, stage)[1:]
        return remote(
            given,
            arrived[array][stage],
            send_sems.at[array, stage],
            recv_sems.at[array, stage],
            (other, column_index),
        )

    def spread(array, step, receiving):
        other = lax.rem(column_index + step, column_parts)
        slot = other if receiving else column_index
        return remote(
            outgoing[array].at[other],
            incoming[array].at[slot],
            send_sems.at[array, row_bits + other],
            recv_sems.at[array, row_bits + slot],
            (row_index, other),
        )

    own_bits = [partner_of(row_index, bit)[0] for bit in range(row_bits - 1, -1, -1)]

    def factor_swap(stage):
        known = (column_index,) + tuple(own_bits[: row_bits - stage])
        return remote(
            factor_out.at[known],
            factor_out.at[known],
            factor_send.at[stage],
            factor_recv.at[stage],
            (partner_of(row_index, stage)[1], column_index),
        )

    def factor_arrival(stage):
        other_bits = own_bits[: row_bits - stage - 1] + [1 - own_bits[row_bits - stage - 1]]
        there = (column_index,) + tuple(other_bits)
        return remote(
            factor_out.at[there],
            factor_out.at[there],
            factor_send.at[stage],
            factor_recv.at[stage],
            (partner_of(row_index, stage)[1], column_index),
        )

    def factor_spread(step, receiving):
        other = lax.rem(column_index + step, column_parts)
        slot = other if receiving else column_index
        return remote(
            factor_out.at[slot],
            factor_out.at[slot],
            factor_send.at[row_bits + other],
            factor_recv.at[row_bits + slot],
            (row_index, other),
        )

    factor_out[(column_index,) + tuple(own_bits)] = factor_in[...]
    greet(row_index, column_index, row_bits, column_parts)
    for array in range(count):
        swap(array, 0).start()
    factor_swap(0).start()
    for stage in range(row_bits):
        for array in range(count):
            copy = swap(array, stage)
            copy.wait_recv()
            copy.wait_send()
            add_tiles(summed[array][stage], halves(array, stage)[0], arrived[array][stage])
            if stage + 1 < row_bits:
                swap(array, stage + 1).start()
                continue
            result = summed[array][stage]
            prefix = plan[array][0]
            parts = outgoing[array]
            for column in range(column_parts):
                if prefix:
                    held = parts.shape[1]
                    for place in range(held):
                        parts[column, place] = result[owners_ref[column * held + place]]
                else:
                    width = parts.shape[-1]
                    parts[column] = result[:, column * width : (column + 1) * width]
            for step in range(1, column_parts):
                spread(array, step, False).start()
        factor_arrival(stage).wait_recv()
        factor_swap(stage).wait_send()
        if stage + 1 < row_bits:
            factor_swap(stage + 1).start()
        else:
            for step in range(1, column_parts):
                factor_spread(step, False).start()
    for array in range(count):
        total = outgoing[array][column_index].astype(jnp.float32)
        for step in range(1, column_parts):
            spread(array, step, True).wait_recv()
            slot = lax.rem(column_index + step, column_parts)
            total = total + incoming[array][slot].astype(jnp.float32)
        outputs[array][...] = total
        for step in range(1, column_parts):
            spread(array, step, False).wait_send()
    for step in range(1, column_parts):
        factor_spread(step, True).wait_recv()
        factor_spread(step, False).wait_send()


def reduce_all(arrays, prefixes, forwards, factors, owners, row_parts, column_parts):
    row_bits = bit_count(row_parts)
    plan = list(zip(prefixes, forwards))
    vmem = pl.BlockSpec(memory_space=pltpu.VMEM)
    scratch, shapes = [], []
    for value, prefix in zip(arrays, prefixes):
        lead, tail = value.shape[:prefix], value.shape[-2:]
        stages = [lead + (2,) * (row_bits - 1 - stage) + tail for stage in range(row_bits)]
        scratch += [pltpu.VMEM(shape, jnp.bfloat16) for shape in stages] * 2
        if prefix:
            part = (lead[0] // column_parts,) + tail
        else:
            part = (tail[0], tail[1] // column_parts)
        scratch += [pltpu.VMEM((column_parts,) + part, jnp.bfloat16)] * 2
        shapes.append(jax.ShapeDtypeStruct(part, jnp.float32))
    shapes.append(
        jax.ShapeDtypeStruct(
            (column_parts,) + (2,) * row_bits + factors.shape, factors.dtype
        )
    )
    count = len(arrays)
    scratch += [
        pltpu.SemaphoreType.DMA((count, row_bits + column_parts)),
        pltpu.SemaphoreType.DMA((count, row_bits + column_parts)),
        pltpu.SemaphoreType.DMA((row_bits + column_parts,)),
        pltpu.SemaphoreType.DMA((row_bits + column_parts,)),
    ]
    return pl.pallas_call(
        partial(reduce_kernel, plan, row_bits, column_parts),
        in_specs=[pl.BlockSpec(memory_space=pltpu.SMEM)] + [vmem] * (count + 1),
        out_specs=[vmem] * (count + 1),
        out_shape=shapes,
        scratch_shapes=scratch,
        compiler_params=pltpu.CompilerParams(
            collective_id=1, has_side_effects=True, vmem_limit_bytes=60 * 1024 * 1024
        ),
        name="reduce_all",
    )(owners, *arrays, factors)


BLOCK = 64


def exact(left, right, left_dim, right_dim):
    return lax.dot_general(
        left,
        right,
        (((left_dim,), (right_dim,)), ((), ())),
        precision=highest,
        preferred_element_type=jnp.float32,
    )


def soap_kernel(
    row_bits,
    column_parts,
    scalars_ref,
    part_ref,
    state_ref,
    grad_ref,
    bases_ref,
    returned_ref,
    totals_ref,
    work,
    small,
    shared,
    direction,
    turned_ref,
    number_send,
    number_recv,
    outgoing,
    number_sems,
    shared_sems,
    return_sems,
):
    held, rows, size = part_ref.shape
    row_parts = 2**row_bits
    column_bits = bit_count(column_parts)
    row_index = lax.axis_index("dp")
    column_index = lax.axis_index("fsdp")
    fix_one, fix_two = scalars_ref[2], scalars_ref[3]
    own_bits = [partner_of(row_index, bit)[0] for bit in range(row_bits - 1, -1, -1)]
    every = slice(None)
    shared[(every,) + tuple(own_bits)] = part_ref[...]
    tile_lane = lax.broadcasted_iota(jnp.int32, (8, 128), 1)
    numbers = jnp.where(
        tile_lane == 0, scalars_ref[0], jnp.where(tile_lane == 1, scalars_ref[1], 0.0)
    )
    number_send[0] = numbers
    greet(row_index, column_index, row_bits, column_parts)

    def number_swap(stage):
        if stage < row_bits:
            device = (partner_of(row_index, stage)[1], column_index)
        else:
            device = (row_index, partner_of(column_index, stage - row_bits)[1])
        return remote(
            number_send.at[stage],
            number_recv.at[stage],
            number_sems.at[0, stage],
            number_sems.at[1, stage],
            device,
        )

    def shared_swap(stage, arriving):
        known = own_bits[: row_bits - stage]
        if arriving:
            known = known[:-1] + [1 - known[-1]]
        place = shared.at[(every,) + tuple(known)]
        device = (partner_of(row_index, stage)[1], column_index)
        return remote(place, place, shared_sems.at[0, stage], shared_sems.at[1, stage], device)

    def early(slot, carry):
        left_basis, right_basis = state_ref[4, slot], state_ref[5, slot]
        turned_ref[slot] = exact(
            exact(left_basis, state_ref[0, slot], 0, 0), right_basis, 1, 0
        )
        work[2 * slot, :, size : 2 * size] = exact(left_basis, state_ref[2, slot], 0, 1)
        work[2 * slot + 1, :, size : 2 * size] = exact(right_basis, state_ref[3, slot], 0, 1)
        return carry

    number_swap(0).start()
    shared_swap(0, False).start()
    rounds = row_bits + column_bits
    for stage in range(rounds):
        if stage < held:
            early(stage, 0)
        number_swap(stage).wait()
        numbers = numbers + number_recv[stage]
        if stage + 1 < rounds:
            number_send[stage + 1] = numbers
        if stage < row_bits:
            shared_swap(stage, True).wait_recv()
            shared_swap(stage, False).wait_send()
            if stage + 1 < row_bits:
                shared_swap(stage + 1, False).start()
        if stage + 1 < rounds:
            number_swap(stage + 1).start()
    totals_ref[...] = numbers
    for slot in range(held):
        for place in range(row_parts):
            bits = tuple((place >> bit) & 1 for bit in range(row_bits - 1, -1, -1))
            grad_ref[slot, place * rows : (place + 1) * rows] = shared[(slot,) + bits]
    norm = jnp.sqrt(numbers[0:1, 0:1])
    clip = jnp.minimum(1.0, clip_limit / norm)

    def prepare(slot, carry):
        gradient = grad_ref[slot] * clip
        grad_ref[slot] = gradient
        left_basis, right_basis = state_ref[4, slot], state_ref[5, slot]
        left_turned = exact(left_basis, gradient, 0, 0)
        right_turned = exact(gradient, right_basis, 1, 0)
        rotated = exact(left_turned, right_basis, 1, 0)
        second = beta_two * state_ref[1, slot] + (1.0 - beta_two) * rotated * rotated
        turned_moment = beta_one * turned_ref[slot] + (1.0 - beta_one) * rotated
        scaled = turned_moment / fix_one / (jnp.sqrt(second / fix_two) + adam_eps)
        direction[slot] = exact(exact(left_basis, scaled, 1, 0), right_basis, 1, 1)
        for side in range(2):
            if side == 0:
                outer = exact(left_turned, gradient, 1, 1)
            else:
                outer = exact(right_turned, gradient, 0, 0)
            place = 2 * slot + side
            image = beta_stat * work[place, :, size : 2 * size] + (1.0 - beta_stat) * outer
            work[place, :, size : 2 * size] = image
            work[place, :, 0:size] = exact(image, image, 1, 1)
        return carry

    lax.fori_loop(0, held, prepare, 0)
    width = size // column_parts
    for slot in range(held):
        mine = jnp.zeros((rows, size), jnp.float32)
        for place in range(row_parts):
            mine = jnp.where(
                row_index == place, direction[slot, place * rows : (place + 1) * rows], mine
            )
        for column in range(column_parts):
            outgoing[column, slot] = mine[:, column * width : (column + 1) * width]

    def give_back(step, receiving):
        other = lax.rem(column_index + step, column_parts)
        slot = other if receiving else column_index
        return remote(
            outgoing.at[other],
            returned_ref.at[slot],
            return_sems.at[0, other],
            return_sems.at[1, slot],
            (row_index, other),
        )

    returned_ref[column_index] = outgoing[column_index]
    for step in range(1, column_parts):
        give_back(step, False).start()
    count = 2 * held
    row = lax.broadcasted_iota(jnp.int32, (BLOCK, 2 * BLOCK), 0)
    lane = lax.broadcasted_iota(jnp.int32, (BLOCK, 2 * BLOCK), 1)
    unit = jnp.where(lane == row + BLOCK, 1.0, 0.0)
    lane_row = lax.broadcasted_iota(jnp.int32, (1, 2 * BLOCK), 1)
    for block in range(size // BLOCK):
        top = block * BLOCK
        for index in range(count):
            diagonal = work[index, top : top + BLOCK, top : top + BLOCK]
            small[index] = unit + jnp.concatenate(
                [diagonal, jnp.zeros((BLOCK, BLOCK), jnp.float32)], axis=1
            )

        def eliminate(half, carry):
            step = 2 * half
            matrices = [small[index] for index in range(count)]
            pairs = [
                (small[index, pl.ds(step, 1), :], small[index, pl.ds(step + 1, 1), :])
                for index in range(count)
            ]
            results = []
            for matrix, (row_one, row_two) in zip(matrices, pairs):
                column_one = jnp.sum(
                    jnp.where(lane == step, matrix, 0.0), axis=1, keepdims=True
                )
                column_two = jnp.sum(
                    jnp.where(lane == step + 1, matrix, 0.0), axis=1, keepdims=True
                )
                corner = jnp.sum(
                    jnp.where(lane_row == step, row_one, 0.0), axis=1, keepdims=True
                )
                cross = jnp.sum(
                    jnp.where(lane_row == step + 1, row_one, 0.0), axis=1, keepdims=True
                )
                last = jnp.sum(
                    jnp.where(lane_row == step + 1, row_two, 0.0), axis=1, keepdims=True
                )
                scale_one = lax.rsqrt(corner)
                slope = cross * scale_one * scale_one
                scale_two = lax.rsqrt(last - slope * cross)
                kept_one = row_one * scale_one
                kept_two = (row_two - slope * row_one) * scale_two
                ratio_one = column_one * scale_one
                ratio_two = (column_two - slope * column_one) * scale_two
                results.append(
                    jnp.where(
                        row > step + 1,
                        matrix - ratio_one * kept_one - ratio_two * kept_two,
                        jnp.where(
                            row == step, kept_one, jnp.where(row == step + 1, kept_two, matrix)
                        ),
                    )
                )
            for index in range(count):
                small[index] = results[index]
            return carry

        lax.fori_loop(0, BLOCK // 2, eliminate, 0)

        def sweep(index, carry):
            inverse = small[index][:, BLOCK : 2 * BLOCK]
            panel = exact(inverse, work[index, top : top + BLOCK, :], 1, 0)
            work[index, top : top + BLOCK, :] = panel
            if top + BLOCK < size:
                lower_part = exact(panel[:, top + BLOCK : size], panel, 0, 0)
                work[index, top + BLOCK : size, :] = (
                    work[index, top + BLOCK : size, :] - lower_part
                )
            return carry

        lax.fori_loop(0, count, sweep, 0)

    def finish(slot, carry):
        for side in range(2):
            bases_ref[side, slot] = work[2 * slot + side, :, size : 2 * size].T
        return carry

    lax.fori_loop(0, held, finish, 0)
    for step in range(1, column_parts):
        give_back(step, True).wait_recv()
        give_back(step, False).wait_send()


def soap_apply(scalars, part, state, row_parts, column_parts):
    held, rows, size = part.shape
    row_bits = bit_count(row_parts)
    rounds = row_bits + bit_count(column_parts)
    square = (held, size, size)
    f32 = jnp.float32
    vmem = pl.BlockSpec(memory_space=pltpu.VMEM)
    moved = (column_parts, held, rows, size // column_parts)
    return pl.pallas_call(
        partial(soap_kernel, row_bits, column_parts),
        in_specs=[pl.BlockSpec(memory_space=pltpu.SMEM), vmem, vmem],
        out_specs=[vmem] * 4,
        out_shape=[
            jax.ShapeDtypeStruct(square, f32),
            jax.ShapeDtypeStruct((2,) + square, f32),
            jax.ShapeDtypeStruct(moved, f32),
            jax.ShapeDtypeStruct((8, 128), f32),
        ],
        scratch_shapes=[
            pltpu.VMEM((2 * held, size, 2 * size), f32),
            pltpu.VMEM((2 * held, BLOCK, 2 * BLOCK), f32),
            pltpu.VMEM((held,) + (2,) * row_bits + (rows, size), f32),
            pltpu.VMEM(square, f32),
            pltpu.VMEM(square, f32),
            pltpu.VMEM((rounds, 8, 128), f32),
            pltpu.VMEM((rounds, 8, 128), f32),
            pltpu.VMEM(moved, f32),
            pltpu.SemaphoreType.DMA((2, rounds)),
            pltpu.SemaphoreType.DMA((2, row_bits)),
            pltpu.SemaphoreType.DMA((2, column_parts)),
        ],
        compiler_params=pltpu.CompilerParams(
            collective_id=2, has_side_effects=True, vmem_limit_bytes=60 * 1024 * 1024
        ),
        name="soap",
    )(scalars, part, state)


def assemble(pieces, row_parts, column_parts):
    height, breadth = pieces.shape[-2:]
    shaped = pieces.reshape(row_parts, column_parts, height, breadth)
    return shaped.transpose(0, 2, 1, 3).reshape(row_parts * height, column_parts * breadth)


def on_device(
    latents,
    noise,
    context,
    timesteps,
    region_mask,
    owners,
    step_count,
    kernels_weight,
    kernels_first,
    kernels_second,
    entry_weight,
    entry_first,
    entry_second,
    middle_weight,
    middle_first,
    middle_second,
    narrow_weight,
    narrow_first,
    narrow_second,
    crossing_weight,
    crossing_first,
    crossing_second,
    widen_weight,
    widen_first,
    widen_second,
    vectors_weight,
    vectors_first,
    vectors_second,
    squares_weight,
    squares_state,
):
    axes = ("dp", "fsdp")
    row_parts = lax.axis_size("dp")
    column_parts = lax.axis_size("fsdp")
    row_index = lax.axis_index("dp")
    column_index = lax.axis_index("fsdp")
    slots = owners.shape[0]

    def gather(value):
        return lax.all_gather(value[None], axes, axis=0, tiled=True)

    def whole(pieces):
        return assemble(pieces, row_parts, column_parts)

    kernel_rows = kernels_weight.shape[1]
    narrow_rows = narrow_weight.shape[1]
    vector_rows = vectors_weight.shape[0]
    square_rows = squares_weight.shape[1]
    tall = [
        kernels_weight[0],
        kernels_weight[1],
        narrow_weight[0],
        narrow_weight[1],
        vectors_weight,
    ] + [squares_weight[index] for index in range(slots)]
    sizes = [piece.shape[0] for piece in tall]
    tall_all = gather(jnp.concatenate([lowered(piece) for piece in tall], axis=0))
    starts = [sum(sizes[:index]) for index in range(len(sizes))]
    tall_full = [
        whole(tall_all[:, start : start + size]) for start, size in zip(starts, sizes)
    ]
    even_all = gather(jnp.concatenate([lowered(entry_weight), lowered(middle_weight)], axis=0))
    entry_rows = entry_weight.shape[0]
    weights = (
        tall_full[0:2],
        whole(even_all[:, :entry_rows]),
        whole(even_all[:, entry_rows:]),
        tall_full[2:4],
        tall_full[4],
        tall_full[5:],
        whole(gather(lowered(crossing_weight))),
        whole(gather(lowered(widen_weight))),
    )
    mask_total = lax.psum(jnp.sum(region_mask.astype(jnp.float32)), axes)
    merged = [
        value.reshape((value.shape[0] * value.shape[1],) + value.shape[2:])
        for value in (latents, noise, context, timesteps, region_mask)
    ]
    loss, kernel_grads, down, crossing, widen, vectors, squares, factors, deltas = device_pass(
        weights, *merged, mask_total
    )
    steps = step_count[0].astype(jnp.float32)
    fix_one = 1.0 - jnp.power(jnp.float32(beta_one), steps)
    fix_two = 1.0 - jnp.power(jnp.float32(beta_two), steps)
    row_bits = bit_count(row_parts)
    halves = (2,) * row_bits
    factor_rows = -(-2 * factors.size // LANES // 16) * 16

    def blocks(value):
        value = lowered(value)
        return value.reshape(halves + (value.shape[0] // row_parts, value.shape[1]))

    vector_blocks = jnp.pad(
        lowered(vectors).reshape(row_parts, vector_rows, C),
        ((0, 0), (0, -vector_rows % 16), (0, 0)),
    )
    packed = jnp.concatenate([factors.reshape(-1), deltas.reshape(-1)])
    packed = jnp.pad(packed, (0, factor_rows * LANES - packed.size)).reshape(factor_rows, LANES)
    (
        kernel_one_part,
        kernel_two_part,
        squares_part,
        widen_part,
        down_part,
        crossing_part,
        vectors_part,
        all_factors,
    ) = reduce_all(
        [
            blocks(kernel_grads[0]),
            blocks(kernel_grads[1]),
            jnp.stack([blocks(piece) for piece in squares]),
            blocks(widen),
            blocks(down),
            blocks(crossing),
            vector_blocks.reshape(halves + vector_blocks.shape[1:]),
        ],
        [0, 0, 1, 0, 0, 0, 0],
        [True, False, True, False, True, False, False],
        packed,
        owners,
        row_parts,
        column_parts,
    )
    gathered = all_factors.reshape(row_parts * column_parts, factor_rows * LANES)
    all_deltas = gathered[:, factors.size : 2 * factors.size].reshape(-1, deltas.shape[1])
    all_factors = gathered[:, : factors.size].reshape(-1, factors.shape[1])

    def outer(row_start, rows, column_start, columns):
        left = lax.dynamic_slice_in_dim(all_factors, row_start + row_index * rows, rows, 1)
        right = lax.dynamic_slice_in_dim(
            all_deltas, column_start + column_index * columns, columns, 1
        )
        return product_left(left, right)

    entry_part = outer(0, entry_weight.shape[0], 0, entry_weight.shape[1])
    middle_part = outer(C, middle_weight.shape[0], 4 * C, middle_weight.shape[1])
    time_part = outer(5 * C, narrow_rows, 8 * C, narrow_weight.shape[2])
    kernels_part = jnp.stack([kernel_one_part, kernel_two_part])
    narrow_part = jnp.stack([time_part, down_part])
    vectors_part = vectors_part[:vector_rows]
    parts = (
        kernels_part,
        entry_part,
        middle_part,
        narrow_part,
        crossing_part,
        widen_part,
        vectors_part,
        squares_part,
    )
    local_square = sum((jnp.sum(piece * piece) for piece in parts))
    squares_grad, squares_slots, returned, both = soap_apply(
        jnp.stack([local_square, loss, fix_one, fix_two]),
        squares_part,
        squares_state,
        row_parts,
        column_parts,
    )
    grad_norm = jnp.sqrt(both[0, 0])
    loss = both[0, 1]
    clip = jnp.minimum(1.0, clip_limit / grad_norm)
    returned = returned.reshape((slots,) + returned.shape[2:])
    picker = (owners[:, None] == jnp.arange(slots)[None, :]).astype(jnp.float32)
    direction_shard = jnp.einsum("sm,sab->mab", picker, returned, precision=highest)
    rate_list = rates()
    squares_master = squares_weight - rate_list[7] * (direction_shard + decay * squares_weight)
    results = []
    for index, (weight, first, second) in enumerate(
        (
            (kernels_weight, kernels_first, kernels_second),
            (entry_weight, entry_first, entry_second),
            (middle_weight, middle_first, middle_second),
            (narrow_weight, narrow_first, narrow_second),
            (crossing_weight, crossing_first, crossing_second),
            (widen_weight, widen_first, widen_second),
            (vectors_weight, vectors_first, vectors_second),
        )
    ):
        results.extend(
            adam(weight, first, second, parts[index] * clip, rate_list[index], fix_one, fix_two)
        )
    totals = jnp.stack([loss, grad_norm])
    return (totals, *results, squares_master, squares_slots, squares_grad)


def solution(mesh):
    return jax.shard_map(
        on_device,
        mesh=mesh,
        in_specs=(
            P(None, ("dp", "fsdp"), None, None),
            P(None, ("dp", "fsdp"), None, None),
            P(None, ("dp", "fsdp"), None, None),
            P(None, ("dp", "fsdp")),
            P(None, ("dp", "fsdp"), None),
            P(),
            P(),
            P(None, "dp", "fsdp"),
            P(None, "dp", "fsdp"),
            P(None, "dp", "fsdp"),
            P("dp", "fsdp"),
            P("dp", "fsdp"),
            P("dp", "fsdp"),
            P("dp", "fsdp"),
            P("dp", "fsdp"),
            P("dp", "fsdp"),
            P(None, "dp", "fsdp"),
            P(None, "dp", "fsdp"),
            P(None, "dp", "fsdp"),
            P("dp", "fsdp"),
            P("dp", "fsdp"),
            P("dp", "fsdp"),
            P("dp", "fsdp"),
            P("dp", "fsdp"),
            P("dp", "fsdp"),
            P("dp", "fsdp"),
            P("dp", "fsdp"),
            P("dp", "fsdp"),
            P(None, "dp", "fsdp"),
            P(None, "fsdp", None, None),
        ),
        out_specs=(
            P(),
            P(None, "dp", "fsdp"),
            P(None, "dp", "fsdp"),
            P(None, "dp", "fsdp"),
            P("dp", "fsdp"),
            P("dp", "fsdp"),
            P("dp", "fsdp"),
            P("dp", "fsdp"),
            P("dp", "fsdp"),
            P("dp", "fsdp"),
            P(None, "dp", "fsdp"),
            P(None, "dp", "fsdp"),
            P(None, "dp", "fsdp"),
            P("dp", "fsdp"),
            P("dp", "fsdp"),
            P("dp", "fsdp"),
            P("dp", "fsdp"),
            P("dp", "fsdp"),
            P("dp", "fsdp"),
            P("dp", "fsdp"),
            P("dp", "fsdp"),
            P("dp", "fsdp"),
            P(None, "dp", "fsdp"),
            P(None, "fsdp", None, None),
            P("fsdp", None, None),
        ),
        check_vma=False,
    )
```
